1024 devices in a mesh: gx: 8 (over z_lo), gy: 32 (over y, z_hi, core), gz: 4 (over x).
Axes of the slice: x: 4, y: 4, z: 32 (z_hi: 4, z_lo: 8; z = z_hi * 8 + z_lo), core: 2. Of those that a mesh axis runs over, the one named last changes fastest.
Arguments:
- positions: float32 [8, 32, 4, 3, 32, 128], P('gx', 'gy', 'gz'), may hold values from 0 to 1
- velocities: float32 [8, 32, 4, 3, 32, 128], P('gx', 'gy', 'gz'), may hold values from -6 to 6
- strength: float32 [8, 32, 4, 32, 128], P('gx', 'gy', 'gz'), may hold values from 0.5 to 2
- tower_slots: int32 [8, 32, 4, 128], P('gx', 'gy', 'gz'), may hold values from 0 to 159
- plate_slots: int32 [8, 32, 4, 128], P('gx', 'gy', 'gz'), may hold values from 0 to 383
- pair_count: int32 [8, 32, 4], P('gx', 'gy', 'gz'), may hold values from 16 to 128, as said below
Outputs:
- new_positions: float32 [8, 32, 4, 3, 32, 128], P('gx', 'gy', 'gz')
- new_velocities: float32 [8, 32, 4, 3, 32, 128], P('gx', 'gy', 'gz')
The draws below stay inside these ranges and needn't reach their ends.
Inputs may be any that keep to these rules, and one draw needn't show every extreme that they name: `pair_count`: slots at or beyond a device's count are padding. Some device has all 128 slots in use.
All inputs are finite; a program needn't handle non-finite values.
Results may differ from the reference program's by a relative error of at most 0.0003.
Values sent between devices are 32-bit elements; how exact they have to be, the bound alone decides.
A program may use at most 32 MiB of HBM per device.

```python
import math
import jax
import jax.numpy as jnp
from jax import lax

CL = 32
CSIZE = 128
PAIR_CAP = 128
N_GX = 8
N_GY = 32
N_GZ = 4


def draw_pair_count(key, part):
    first_key, second_key = jax.random.split(jax.random.fold_in(key, 11))
    halvings = jax.random.randint(first_key, (N_GX, N_GY, N_GZ), 0, 4)
    counts = jnp.right_shift(jnp.full((N_GX, N_GY, N_GZ), PAIR_CAP, jnp.int32), halvings.astype(jnp.int32))
    busiest = jax.random.randint(second_key, (), 0, N_GX * N_GY * N_GZ)
    counts = counts.reshape(-1).at[busiest].set(PAIR_CAP)
    return counts.reshape((N_GX, N_GY, N_GZ)).astype(jnp.int32)


def plant(values, rng, least, high):
    longest = values.shape.index(max(values.shape))
    spots = []
    for shift in (0, 1):
        where = [jax.random.randint(jax.random.fold_in(rng, axis), (), 0, length) for axis, length in enumerate(values.shape)]
        where[longest] = (where[longest] + shift) % values.shape[longest]
        spots.append(tuple(where))
    return values.at[spots[0]].set(least).at[spots[1]].set(high)


def level_of(stream_key, extent, pieces, low, top_value):
    loudness, own = 1.0, jax.random.fold_in(stream_key, 6)
    for dim, parts in pieces:
        steps = jnp.exp(jax.random.uniform(jax.random.fold_in(own, dim), (parts,), jnp.float32, low / len(pieces), top_value / len(pieces)))
        loudness = loudness * jnp.repeat(steps, extent[dim] // parts).reshape([-1 if axis == dim else 1 for axis in range(len(extent))])
    return loudness


def noise(key, extent, deviation, reach, cuts=(), held_as=jnp.bfloat16):
    loudness = level_of(key, extent, cuts, -0.22, 0.18) if cuts else 1.0
    values = jax.random.normal(key, extent, jnp.float32) * deviation * loudness
    return jnp.minimum(jnp.maximum(values, -reach), reach).astype(held_as)


def setup_inputs(seed: int = 0) -> dict:
    splits = jax.random.split(jax.random.key(seed), 7)
    return {
        "positions": jnp.clip(1.0 * jax.random.uniform(splits[0], (N_GX, N_GY, N_GZ, 3, CL, CSIZE), jnp.float32) ** level_of(splits[0], (N_GX, N_GY, N_GZ, 3, CL, CSIZE), ((0, 8), (1, 32), (2, 4)), -0.2, 0.2), 0.0, 1.0),
        "velocities": noise(splits[1], (N_GX, N_GY, N_GZ, 3, CL, CSIZE), 1.0, 6.0, ((0, 8), (1, 32), (2, 4)), jnp.float32),
        "strength": jnp.clip(jnp.exp(math.log(2.0) - 1.3862944 * jax.random.uniform(splits[2], (N_GX, N_GY, N_GZ, CL, CSIZE), jnp.float32) ** level_of(splits[2], (N_GX, N_GY, N_GZ, CL, CSIZE), ((0, 8), (1, 32), (2, 4)), -0.2, 0.2)), 0.5, 2.0),
        "tower_slots": plant(jax.random.randint(splits[3], (N_GX, N_GY, N_GZ, PAIR_CAP), 0, 5 * CL), jax.random.fold_in(splits[3], 1), 0, (5 * CL) - 1).astype(jnp.int32),
        "plate_slots": plant(jax.random.randint(splits[4], (N_GX, N_GY, N_GZ, PAIR_CAP), 0, 3 * N_GZ * CL), jax.random.fold_in(splits[4], 1), 0, (3 * N_GZ * CL) - 1).astype(jnp.int32),
        "pair_count": draw_pair_count(jax.random.fold_in(splits[6], 71), 0),
    }


time_step = 0.02
cutoff_sq = 4.0
repulsion = 4.0
pair_block = 16


def placed_tower(tower_pos, height_level):
    shifts = (jnp.arange(5, dtype=jnp.float32) - 2.0)[:, None, None]
    return jnp.stack([tower_pos[:, 0] + shifts, tower_pos[:, 1], tower_pos[:, 2] + height_level], axis=1)


def placed_plate(plate_pos):
    line_shift = jnp.arange(plate_pos.shape[0], dtype=jnp.float32)[:, None, None, None]
    height_shift = jnp.arange(plate_pos.shape[1], dtype=jnp.float32)[None, :, None, None]
    return jnp.stack([plate_pos[:, :, 0], plate_pos[:, :, 1] + line_shift, plate_pos[:, :, 2] + height_shift], axis=2)


def block_forces(accum, begin_at, tower_pos, tower_str, plate_pos, plate_str, tower_list, plate_list, pair_total):
    tower_force, plate_force = accum
    clusters = tower_pos.shape[2]
    tower_pick = lax.dynamic_slice_in_dim(tower_list, begin_at, pair_block)
    plate_pick = lax.dynamic_slice_in_dim(plate_list, begin_at, pair_block)
    tower_block = tower_pick // clusters
    tower_index = tower_pick % clusters
    plate_block = plate_pick // clusters
    plate_index = plate_pick % clusters
    tower_side = tower_pos[tower_block, :, tower_index, :]
    plate_side = plate_pos[plate_block, :, plate_index, :]
    tower_weight = tower_str[tower_block, tower_index]
    plate_weight = plate_str[plate_block, plate_index]
    live_mask = (begin_at + jnp.arange(pair_block, dtype=jnp.int32) < pair_total).astype(jnp.float32)
    separation = tower_side[:, :, :, None] - plate_side[:, :, None, :]
    dist_sq = jnp.sum(separation * separation, axis=1)
    softness = jnp.maximum(1.0 - dist_sq / cutoff_sq, 0.0)
    weight = repulsion * softness * softness * tower_weight[:, :, None] * plate_weight[:, None, :] * live_mask[:, None, None]
    pair_push = weight[:, None] * separation
    tower_force = tower_force.at[tower_block, :, tower_index, :].add(jnp.sum(pair_push, axis=3))
    plate_force = plate_force.at[plate_block, :, plate_index, :].add(-jnp.sum(pair_push, axis=2))
    return tower_force, plate_force


def total_force(coords, strength, tower_slots, plate_slots, pair_count):
    rows_total = coords.shape[0]
    lines_total = coords.shape[1]
    heights_total = coords.shape[2]

    def column(accum, column_id):
        row_index = column_id // lines_total
        line_index = column_id % lines_total
        tower_all = jnp.stack([coords[(row_index + offset) % rows_total, line_index] for offset in (-2, -1, 0, 1, 2)])
        tower_str_all = jnp.stack([strength[(row_index + offset) % rows_total, line_index] for offset in (-2, -1, 0, 1, 2)])
        plate_all = jnp.stack([coords[row_index, (line_index + offset) % lines_total] for offset in (0, 1, 2)])
        plate_str_all = jnp.stack([strength[row_index, (line_index + offset) % lines_total] for offset in (0, 1, 2)])
        plate_flat = placed_plate(plate_all).reshape((3 * heights_total,) + plate_all.shape[2:])
        plate_str_flat = plate_str_all.reshape((3 * heights_total,) + plate_str_all.shape[2:])

        def one_height(height_id):
            tower_here = placed_tower(tower_all[:, height_id], height_id.astype(jnp.float32))
            tower_str_here = tower_str_all[:, height_id]
            tower_list = tower_slots[row_index, line_index, height_id]
            plate_list = plate_slots[row_index, line_index, height_id]
            pair_total = pair_count[row_index, line_index, height_id]
            start_force = (jnp.zeros(tower_here.shape, jnp.float32), jnp.zeros(plate_flat.shape, jnp.float32))

            def advance(block_id, state):
                return block_forces(state, block_id * pair_block, tower_here, tower_str_here, plate_flat, plate_str_flat, tower_list, plate_list, pair_total)

            return lax.fori_loop(0, PAIR_CAP // pair_block, advance, start_force)

        tower_force, plate_force = lax.map(one_height, jnp.arange(heights_total, dtype=jnp.int32))
        plate_sum = jnp.sum(plate_force, axis=0).reshape((3, heights_total) + plate_all.shape[2:])
        for offset in (-2, -1, 0, 1, 2):
            accum = accum.at[(row_index + offset) % rows_total, line_index].add(tower_force[:, offset + 2])
        for offset in (0, 1, 2):
            accum = accum.at[row_index, (line_index + offset) % lines_total].add(plate_sum[offset])
        return accum, None

    result, unused = lax.scan(column, jnp.zeros(coords.shape, jnp.float32), jnp.arange(rows_total * lines_total, dtype=jnp.int32))
    return result


def reference(positions, velocities, strength, tower_slots, plate_slots, pair_count):
    coords = positions
    speeds = velocities
    for leap_index in range(2):
        force = total_force(coords, strength, tower_slots, plate_slots, pair_count)
        speeds = speeds + time_step * force
        coords = coords + time_step * speeds
    return coords, speeds
```

```python
import functools

import jax
import jax.numpy as jnp
from jax import lax
from jax.experimental import pallas as pl
from jax.experimental.pallas import tpu as pltpu
from jax.sharding import PartitionSpec as P

time_step = 0.02
CL = 32
CS = 128
PAIRS = 128
GROUP = 8
MESH = pl.DeviceIdType.MESH
COPIES = 32
F32 = jnp.float32
BF16 = jnp.bfloat16


def rounded(v):
    return v.astype(BF16).astype(F32)


def split3(v):
    a = rounded(v)
    r = v - a
    b = rounded(r)
    return a, b, rounded(r - b)


def features(rows, weight, sub):
    sq = rows * rows
    norm = (sq[0:1] + sq[1:2] + sq[2:3]) * 0.25
    scaled = rows * weight
    high = rounded(scaled)
    sums = jnp.concatenate([high, scaled - high], axis=0).astype(BF16)
    return norm, sums


def gather_side(pos, wts, block, index, shift, sub):
    x = jnp.broadcast_to(pos[block, 0, pl.ds(index, 1), :], (8, CS))
    y = jnp.broadcast_to(pos[block, 1, pl.ds(index, 1), :], (8, CS))
    z = jnp.broadcast_to(pos[block, 2, pl.ds(index, 1), :], (8, CS))
    s = jnp.broadcast_to(wts[block, 3, pl.ds(index, 1), :], (8, CS))
    one = jnp.where(sub == 3, 1.0, 0.0)
    rows = jnp.where(sub == 0, x, jnp.where(sub == 1, y, jnp.where(sub == 2, z, one)))
    if shift is not None:
        rows = rows + shift
    return rows, s


def one_pair(n, tower, wt_tower, plate, wt_plate, t_slots, p_slots, height, sub):
    ts = t_slots[0, n]
    ps = p_slots[0, n]
    t_block = lax.shift_right_logical(ts, 5)
    t_index = lax.bitwise_and(ts, 31)
    p_block = lax.shift_right_logical(ps, 5)
    p_index = lax.bitwise_and(ps, 31)
    dx = (t_block - 2).astype(F32)
    dy = -lax.shift_right_logical(ps, 7).astype(F32)
    dz = (height - lax.bitwise_and(p_block, 3)).astype(F32)
    shift = jnp.where(sub == 0, dx, jnp.where(sub == 1, dy, jnp.where(sub == 2, dz, 0.0)))
    a, sa = gather_side(tower, wt_tower, t_block, t_index, shift, sub)
    q, sq = gather_side(plate, wt_plate, p_block, p_index, None, sub)
    norm_a, sums_a = features(a, sa, sub)
    norm_q, sums_q = features(q, sq, sub)
    left = jnp.where(
        sub < 3, 0.5 * a, jnp.where(sub == 3, 1.0 - norm_a, jnp.where(sub == 4, 1.0, 0.0))
    )
    right = jnp.where(sub == 4, -norm_q, q)
    a1, a2, a3 = split3(left)
    q1, q2, q3 = split3(right)
    lhs = jnp.concatenate([a1, a1, a2, a1, a3, a2], axis=0)
    rhs = jnp.concatenate([q1, q2, q1, q3, q1, q2], axis=0)
    return dict(a=a, sa=sa, q=q, sq=sq, sums_a=sums_a, sums_q=sums_q, lhs=lhs, rhs=rhs)


def dot(a, b, dims):
    return lax.dot_general(a, b, (dims, ((), ())), preferred_element_type=F32)


def two_pairs(first, n, fa_ref, fq_ref):
    u, v = first
    lhs = jnp.concatenate([u["lhs"], v["lhs"]], axis=0)
    lhs = lhs.T.astype(BF16)
    zero = jnp.zeros((48, CS), F32)
    rhs = jnp.concatenate(
        [jnp.concatenate([u["rhs"], zero], axis=1), jnp.concatenate([zero, v["rhs"]], axis=1)],
        axis=0,
    ).astype(BF16)
    t = dot(lhs, rhs, ((1,), (0,)))
    m = jnp.maximum(t, 0.0)
    m = (m * m).astype(BF16)
    wa = jnp.concatenate([u["sums_a"], v["sums_a"]], axis=0)
    wq = jnp.concatenate([u["sums_q"], v["sums_q"]], axis=0)
    on_q = dot(wa, m, ((1,), (0,)))
    stacked = jnp.concatenate([m[:, :CS], m[:, CS:]], axis=0)
    on_a = dot(wq, stacked, ((1,), (1,)))
    for k, w in enumerate((u, v)):
        cols = slice(k * CS, (k + 1) * CS)
        for rows, weight, out, ref in (
            (w["a"], w["sa"], on_a, fa_ref),
            (w["q"], w["sq"], on_q, fq_ref),
        ):
            got = out[16 * k : 16 * k + 8, cols] + out[16 * k + 8 : 16 * k + 16, cols]
            force = (rows * got[3:4] - got) * (4.0 * weight)
            for c in range(3):
                ref[c, pl.ds(n + k, 1), :] = force[c : c + 1]


def spread(pair_forces, slots, live, count, out_ref, blocks):
    rows = blocks * CL
    which = lax.broadcasted_iota(jnp.int32, (rows, PAIRS), 0)
    pick = jnp.where((which == slots) & (live < count), 1.0, 0.0).astype(BF16)
    pick = jnp.concatenate([pick, pick], axis=1)
    for c in range(3):
        v = pair_forces[c]
        high = rounded(v)
        both = jnp.concatenate([high, v - high], axis=0).astype(BF16)
        out_ref[:, c] = dot(pick, both, ((1,), (0,))).reshape(blocks, CL, CS)


def kernel(
    pos_ref, vel_ref, str_ref, ts_ref, ps_ref, cnt_ref, tv_ref, pv_ref,
    out_pos, out_vel,
    plate0, plate1, tower0, tower1, pf0, pf1, tf0, tf1, rt0, rt1, rd0, rd1, rx0, rx1,
    line0, line1, rl0, rl1, fa_ref, fq_ref, now, send, recv,
):
    i = lax.axis_index("gx")
    j = lax.axis_index("gy")
    k = lax.axis_index("gz")
    nx, ny, nz = lax.axis_size("gx"), lax.axis_size("gy"), lax.axis_size("gz")
    core = lax.rem(j, 2)
    at_x = lambda d: {"gx": lax.rem(i + d + nx, nx)}
    at_y = lambda d: {"gy": lax.rem(j + d + ny, ny)}
    at_z = lambda d: {"gz": lax.rem(k + d + nz, nz)}
    partner = {"gy": j + 1 - 2 * core}

    barrier = pltpu.get_barrier_semaphore()
    peers = [at_x(d) for d in (-2, -1, 1, 2)] + [at_y(-2), at_y(2), partner]
    peers += [at_z(d) for d in (1, 2, 3)]
    for peer in peers:
        pl.semaphore_signal(barrier, inc=1, device_id=peer, device_id_type=MESH)

    plate0[k, 0:3] = pos_ref[...]
    plate0[k, 3] = str_ref[...]
    tower0[2, 0:3] = pos_ref[...]
    tower0[2, 3] = str_ref[...]
    now[0] = pos_ref[...]
    now[1] = vel_ref[...]
    pl.semaphore_wait(barrier, len(peers))

    sub = lax.broadcasted_iota(jnp.int32, (8, CS), 0)
    live = lax.broadcasted_iota(jnp.int32, (1, PAIRS), 1)
    count = cnt_ref[0, 0]
    started = []

    def push(leap, number, src, dst, where):
        copy = pltpu.make_async_remote_copy(
            src_ref=src, dst_ref=dst,
            send_sem=send.at[leap, number], recv_sem=recv.at[leap, number],
            device_id=where, device_id_type=MESH,
        )
        copy.start()
        started.append(copy)
        return copy

    for leap in range(2):
        plate, tower = ((plate0, tower0), (plate1, tower1))[leap]
        pf, tf = ((pf0, tf0), (pf1, tf1))[leap]
        rt, rd, rx = ((rt0, rd0, rx0), (rt1, rd1, rx1))[leap]
        line, rl = ((line0, rl0), (line1, rl1))[leap]
        go = functools.partial(push, leap)

        line_in = go(0, plate.at[k], plate.at[2 * nz + k], at_y(-2))
        tower_in = [
            go(1 + s, plate.at[k], tower.at[2 + d], at_x(-d)) for s, d in enumerate((-2, 2, -1, 1))
        ]
        own_in = [go(5 + r, plate.at[k], plate.at[k], at_z(r)) for r in (1, 2, 3)]
        source = 2 * nz * (1 - core)

        height = lambda r: lax.rem(k - r + nz, nz)

        def share_if(who, r, plate=plate, leap=leap):
            @pl.when(core == who)
            def _():
                pltpu.make_async_remote_copy(
                    src_ref=plate.at[source + height(r)], dst_ref=plate.at[nz + height(r)],
                    send_sem=send.at[leap, 12 + r], recv_sem=recv.at[leap, 12 + r],
                    device_id=partner, device_id_type=MESH,
                ).start()

        share_if(1, 0)
        for r in (1, 2, 3):
            own_in[r - 1].wait_recv()
            share_if(1, r)
        line_in.wait_recv()
        far_in = [go(8 + r, plate.at[2 * nz + k], plate.at[2 * nz + k], at_z(r)) for r in (1, 2, 3)]
        share_if(0, 0)
        for r in (1, 2, 3):
            far_in[r - 1].wait_recv()
            share_if(0, r)
        for r in range(4):
            copy = pltpu.make_async_remote_copy(
                src_ref=plate.at[source + height(r)], dst_ref=plate.at[nz + height(r)],
                send_sem=send.at[leap, 12 + r], recv_sem=recv.at[leap, 12 + r],
                device_id=partner, device_id_type=MESH,
            )
            started.append(copy)
            copy.wait_recv()
        for copy in tower_in:
            copy.wait_recv()

        def pairs(g, carry, tower=tower, plate=plate):
            base = g * GROUP
            for two in range(GROUP // 2):
                n = base + 2 * two
                both = [
                    one_pair(n + w, tower, tower0, plate, plate0, ts_ref, ps_ref, k, sub)
                    for w in range(2)
                ]
                two_pairs(both, n, fa_ref, fq_ref)
            return carry

        lax.fori_loop(0, PAIRS // GROUP, pairs, 0)
        spread(fq_ref, pv_ref[...], live, count, pf, 3 * 4)
        spread(fa_ref, tv_ref[...], live, count, tf, 5)

        mid = go(16, pf.at[pl.ds(nz, nz)], rd, partner)
        rows_in = [
            go(17 + s, tf.at[2 + d], rt.at[s], at_x(d)) for s, d in enumerate((-2, 2, -1, 1))
        ]
        first = 2 * nz * core
        second = 2 * nz * (1 - core)
        early = [
            go(20 + r, pf.at[first + lax.rem(k + r, nz)], rx.at[r - 1], at_z(r)) for r in (1, 2, 3)
        ]
        mid.wait_recv()
        pf[pl.ds(second, nz)] = pf[pl.ds(second, nz)] + rd[...]
        late = [
            go(23 + r, pf.at[second + lax.rem(k + r, nz)], rx.at[2 + r], at_z(r))
            for r in (1, 2, 3)
        ]
        for copy in early:
            copy.wait_recv()
        sum_early = pf[first + k] + rx[0] + rx[1] + rx[2]
        for copy in late:
            copy.wait_recv()
        sum_late = pf[second + k] + rx[3] + rx[4] + rx[5]
        is_even = core == 0
        line[...] = jnp.where(is_even, sum_late, sum_early)
        home = go(27, line, rl, at_y(2))
        force = jnp.where(is_even, sum_early, sum_late) + tf[2]
        for copy in rows_in:
            copy.wait_recv()
        force = force + rt[0] + rt[1] + rt[2] + rt[3]
        home.wait_recv()
        force = force + rl[...]
        speed = now[1] + time_step * force
        place = now[0] + time_step * speed
        if leap == 0:
            now[1] = speed
            now[0] = place
            plate1[k] = place
            tower1[2] = place
        else:
            out_vel[...] = speed
            out_pos[...] = place
    for copy in started:
        copy.wait_send()


def shards(positions, velocities, strength, tower_slots, plate_slots, pair_count):
    vm = pl.BlockSpec(memory_space=pltpu.VMEM)
    sm = pl.BlockSpec(memory_space=pltpu.SMEM)
    block = (3, CL, CS)
    scratch = []
    for shape in ((12, 4, CL, CS), (12, *block), (5, 4, CL, CS), (5, *block)):
        scratch.append(pltpu.VMEM(shape, F32))
    for blocks in (12, 5, 4, 4, 6):
        scratch += [pltpu.VMEM((blocks, *block), F32)] * 2
    scratch += [pltpu.VMEM(block, F32)] * 4
    scratch += [pltpu.VMEM((3, PAIRS, CS), F32)] * 2
    scratch += [pltpu.VMEM((2, *block), F32)]
    scratch += [pltpu.SemaphoreType.DMA((2, COPIES))] * 2
    tower_slots = tower_slots.reshape(1, PAIRS)
    plate_slots = plate_slots.reshape(1, PAIRS)
    new_pos, new_vel = pl.pallas_call(
        kernel,
        out_shape=[jax.ShapeDtypeStruct(block, F32)] * 2,
        in_specs=[vm, vm, vm, sm, sm, sm, vm, vm],
        out_specs=[vm, vm],
        scratch_shapes=scratch,
        compiler_params=pltpu.CompilerParams(collective_id=0, has_side_effects=True),
        name="leapfrog",
    )(
        positions.reshape(block), velocities.reshape(block), strength.reshape(CL, CS),
        tower_slots, plate_slots, pair_count.reshape(1, 1), tower_slots, plate_slots,
    )
    return new_pos[None, None, None], new_vel[None, None, None]


def solution(mesh):
    wide = P("gx", "gy", "gz", None, None, None)
    in_specs = (
        wide, wide, P("gx", "gy", "gz", None, None),
        P("gx", "gy", "gz", None), P("gx", "gy", "gz", None), P("gx", "gy", "gz"),
    )
    return jax.shard_map(
        shards, mesh=mesh, in_specs=in_specs, out_specs=(wide, wide), check_vma=False
    )
```

```python
import jax
import jax.numpy as jnp
from jax import lax
from jax.experimental import pallas as pl
from jax.experimental.pallas import tpu as pltpu
from jax.sharding import PartitionSpec as P

time_step = 0.02
CL = 32
CS = 128
PAIRS = 128
GROUP = 32
PARTS = 2
ROWS = CL // PARTS
MESH = pl.DeviceIdType.MESH
COPIES = 28
F32 = jnp.float32
BF16 = jnp.bfloat16


def rounded(v):
    return v.astype(BF16).astype(F32)


def split3(v):
    a = rounded(v)
    r = v - a
    b = rounded(r)
    return a, b, rounded(r - b)


def features(rows, weight, sub):
    sq = rows * rows
    norm = (sq[0:1] + sq[1:2] + sq[2:3]) * 0.25
    scaled = rows * weight
    high = rounded(scaled)
    sums = jnp.concatenate([high, scaled - high], axis=0).astype(BF16)
    return norm, sums


def gather_side(pos, wts, block, index, shift, sub):
    x = jnp.broadcast_to(pos[block, 0, pl.ds(index, 1), :], (8, CS))
    y = jnp.broadcast_to(pos[block, 1, pl.ds(index, 1), :], (8, CS))
    z = jnp.broadcast_to(pos[block, 2, pl.ds(index, 1), :], (8, CS))
    s = jnp.broadcast_to(wts[block, 3, pl.ds(index, 1), :], (8, CS))
    one = jnp.where(sub == 3, 1.0, 0.0)
    rows = jnp.where(sub == 0, x, jnp.where(sub == 1, y, jnp.where(sub == 2, z, one)))
    if shift is not None:
        rows = rows + shift
    return rows, s


def one_pair(n, tower, wt_tower, plate, wt_plate, t_slots, p_slots, height, sub):
    ts = t_slots[0, n]
    ps = p_slots[0, n]
    t_block = lax.shift_right_logical(ts, 5)
    t_index = lax.bitwise_and(ts, 31)
    p_block = lax.shift_right_logical(ps, 5)
    p_index = lax.bitwise_and(ps, 31)
    dx = (t_block - 2).astype(F32)
    dy = -lax.shift_right_logical(ps, 7).astype(F32)
    dz = (height - lax.bitwise_and(p_block, 3)).astype(F32)
    shift = jnp.where(sub == 0, dx, jnp.where(sub == 1, dy, jnp.where(sub == 2, dz, 0.0)))
    a, sa = gather_side(tower, wt_tower, t_block, t_index, shift, sub)
    q, sq = gather_side(plate, wt_plate, p_block, p_index, None, sub)
    norm_a, sums_a = features(a, sa, sub)
    norm_q, sums_q = features(q, sq, sub)
    left = jnp.where(
        sub < 3, 0.5 * a, jnp.where(sub == 3, 1.0 - norm_a, jnp.where(sub == 4, 1.0, 0.0))
    )
    right = jnp.where(sub == 4, -norm_q, q)
    a1, a2, a3 = split3(left)
    q1, q2, q3 = split3(right)
    lhs = jnp.concatenate([a1, a1, a2, a1, a3, a2], axis=0)
    rhs = jnp.concatenate([q1, q2, q1, q3, q1, q2], axis=0)
    return dict(a=a, sa=sa, q=q, sq=sq, sums_a=sums_a, sums_q=sums_q, lhs=lhs, rhs=rhs)


def dot(a, b, dims):
    return lax.dot_general(a, b, (dims, ((), ())), preferred_element_type=F32)


def beside(u, v):
    lhs = jnp.concatenate([u["lhs"], v["lhs"]], axis=0).T.astype(BF16)
    zero = jnp.zeros((48, CS), F32)
    rhs = jnp.concatenate(
        [jnp.concatenate([u["rhs"], zero], axis=1), jnp.concatenate([zero, v["rhs"]], axis=1)],
        axis=0,
    ).astype(BF16)
    return lhs, rhs


def group_of_pairs(sides, n, fa_ref, fq_ref):
    twos = [sides[w : w + 2] for w in range(0, len(sides), 2)]
    products = [beside(u, v) for u, v in twos]
    ts = [dot(lhs, rhs, ((1,), (0,))) for lhs, rhs in products]
    outs = []
    for (u, v), t in zip(twos, ts):
        m = jnp.maximum(t, 0.0)
        m = (m * m).astype(BF16)
        wa = jnp.concatenate([u["sums_a"], v["sums_a"]], axis=0)
        wq = jnp.concatenate([u["sums_q"], v["sums_q"]], axis=0)
        stacked = jnp.concatenate([m[:, :CS], m[:, CS:]], axis=0)
        outs.append((dot(wq, stacked, ((1,), (1,))), dot(wa, m, ((1,), (0,)))))
    for w, side in enumerate(sides):
        half = w % 2
        cols = slice(half * CS, (half + 1) * CS)
        on_a, on_q = outs[w // 2]
        for rows, weight, out, ref in (
            (side["a"], side["sa"], on_a, fa_ref),
            (side["q"], side["sq"], on_q, fq_ref),
        ):
            got = out[16 * half : 16 * half + 8, cols] + out[16 * half + 8 : 16 * half + 16, cols]
            force = (rows * got[3:4] - got) * (4.0 * weight)
            for c in range(3):
                ref[c, pl.ds(n + w, 1), :] = force[c : c + 1]


def spread(pair_forces, slots, live, count, out_ref, blocks):
    rows = blocks * CL
    which = lax.broadcasted_iota(jnp.int32, (rows, PAIRS), 0)
    pick = jnp.where((which == slots) & (live < count), 1.0, 0.0).astype(BF16)
    pick = jnp.concatenate([pick, pick], axis=1)
    for c in range(3):
        v = pair_forces[c]
        high = rounded(v)
        both = jnp.concatenate([high, v - high], axis=0).astype(BF16)
        out_ref[:, c] = dot(pick, both, ((1,), (0,))).reshape(blocks, CL, CS)


def kernel(
    pos_ref, vel_ref, str_ref, ts_ref, ps_ref, cnt_ref, tv_ref, pv_ref,
    out_pos, out_vel,
    plate0, plate1, tower0, tower1, pf0, pf1, tf0, tf1, rt0, rt1, rd0, rd1, rx0, rx1,
    line0, line1, rl0, rl1, fa_ref, fq_ref, now, send, recv,
):
    i = lax.axis_index("gx")
    j = lax.axis_index("gy")
    k = lax.axis_index("gz")
    nx, ny, nz = lax.axis_size("gx"), lax.axis_size("gy"), lax.axis_size("gz")
    core = lax.rem(j, 2)
    at_x = lambda d: {"gx": lax.rem(i + d + nx, nx)}
    at_y = lambda d: {"gy": lax.rem(j + d + ny, ny)}
    at_z = lambda d: {"gz": lax.rem(k + d + nz, nz)}
    partner = {"gy": j + 1 - 2 * core}
    steps = ((0, -2), (1, 2), (2, -1), (3, 1))

    barrier = pltpu.get_barrier_semaphore()
    peers = [at_x(d) for d in (-2, -1, 1, 2)] + [at_y(-2), at_y(2), partner]
    peers += [at_z(d) for d in (1, 2, 3)]
    for peer in peers:
        pl.semaphore_signal(barrier, inc=1, device_id=peer, device_id_type=MESH)

    plate0[k, 0:3] = pos_ref[...]
    plate0[k, 3] = str_ref[...]
    tower0[2, 0:3] = pos_ref[...]
    tower0[2, 3] = str_ref[...]
    now[0] = pos_ref[...]
    now[1] = vel_ref[...]
    with jax.named_scope("barrier"):
        pl.semaphore_wait(barrier, len(peers))

    sub = lax.broadcasted_iota(jnp.int32, (8, CS), 0)
    live = lax.broadcasted_iota(jnp.int32, (1, PAIRS), 1)
    count = cnt_ref[0, 0]
    started = []

    def copy_of(leap, part, number, src, dst, where):
        return pltpu.make_async_remote_copy(
            src_ref=src, dst_ref=dst,
            send_sem=send.at[leap, part, number], recv_sem=recv.at[leap, part, number],
            device_id=where, device_id_type=MESH,
        )

    def go(*args):
        copy = copy_of(*args)
        copy.start()
        started.append(copy)
        return copy

    def rows(part):
        return pl.ds(part * ROWS, ROWS)

    def await_all(copies, name):
        for copy in copies:
            with jax.named_scope(name):
                copy.wait_recv()

    def send_line(leap, part, plate):
        r = rows(part)
        return go(leap, part, 0, plate.at[k, :, r], plate.at[2 * nz + k, :, r], at_y(-2))

    def send_tower(leap, part, plate, tower):
        r = rows(part)
        return [
            go(leap, part, 1 + s, plate.at[k, :, r], tower.at[2 + d, :, r], at_x(-d))
            for s, d in steps
        ]

    def send_over(leap, part, plate, number, block):
        r = rows(part)
        return [
            go(leap, part, number + d, plate.at[block, :, r], plate.at[block, :, r], at_z(d + 1))
            for d in range(3)
        ]

    def shared(leap, part, plate, d):
        height = lax.rem(k - d + nz, nz)
        r = rows(part)
        return copy_of(
            leap, part, 11 + d,
            plate.at[2 * nz * (1 - core) + height, :, r], plate.at[nz + height, :, r], partner,
        )

    def share_if(who, *args):
        @pl.when(core == who)
        def _():
            shared(*args).start()

    parts = range(PARTS)
    line_in = [send_line(0, part, plate0) for part in parts]
    own_in = [send_over(0, part, plate0, 5, k) for part in parts]
    tower_in = [send_tower(0, part, plate0, tower0) for part in parts]
    for leap in range(2):
        plate, tower = ((plate0, tower0), (plate1, tower1))[leap]
        pf, tf = ((pf0, tf0), (pf1, tf1))[leap]
        rt, rd, rx = ((rt0, rd0, rx0), (rt1, rd1, rx1))[leap]
        line, rl = ((line0, rl0), (line1, rl1))[leap]

        for part in parts:
            share_if(1, leap, part, plate, 0)
            for d in range(3):
                await_all([own_in[part][d]], f"own{leap}")
                share_if(1, leap, part, plate, d + 1)
        far_in = []
        for part in parts:
            await_all([line_in[part]], f"line{leap}")
            far_in.append(send_over(leap, part, plate, 8, 2 * nz + k))
            share_if(0, leap, part, plate, 0)
        for part in parts:
            for d in range(3):
                await_all([far_in[part][d]], f"far{leap}")
                share_if(0, leap, part, plate, d + 1)
        between = [shared(leap, part, plate, d) for part in parts for d in range(nz)]
        started += between
        await_all(between, f"mid{leap}")
        for part in parts:
            await_all(tower_in[part], f"tower{leap}")

        def pairs(g, carry, tower=tower, plate=plate):
            base = g * GROUP
            sides = [
                one_pair(base + w, tower, tower0, plate, plate0, ts_ref, ps_ref, k, sub)
                for w in range(GROUP)
            ]
            group_of_pairs(sides, base, fa_ref, fq_ref)
            return carry

        with jax.named_scope(f"pairs{leap}"):
            lax.fori_loop(0, PAIRS // GROUP, pairs, 0)
        with jax.named_scope(f"spread{leap}"):
            spread(fq_ref, pv_ref[...], live, count, pf, 3 * 4)
            spread(fa_ref, tv_ref[...], live, count, tf, 5)

        first = 2 * nz * core
        second = 2 * nz * (1 - core)

        def over(part, number, block, slot, leap=leap, pf=pf, rx=rx):
            r = rows(part)
            return [
                go(
                    leap, part, number + d, pf.at[block + lax.rem(k + d + 1, nz), :, r],
                    rx.at[slot + d, :, r], at_z(d + 1),
                )
                for d in range(3)
            ]

        mid, early, rows_in, late, home = [], [], [], [], []
        for part in parts:
            r = rows(part)
            mid.append(go(leap, part, 15, pf.at[pl.ds(nz, nz), :, r], rd.at[:, :, r], partner))
            early.append(over(part, 20, first, 0))
            rows_in.append([
                go(leap, part, 16 + s, tf.at[2 + d, :, r], rt.at[s, :, r], at_x(d))
                for s, d in steps
            ])
        for part in parts:
            r = rows(part)
            await_all([mid[part]], f"rmid{leap}")
            pf[pl.ds(second, nz), :, r] = pf[pl.ds(second, nz), :, r] + rd[:, :, r]
            late.append(over(part, 23, second, 3))
        keep = []
        for part in parts:
            r = rows(part)
            await_all(early[part], f"early{leap}")
            sum_early = pf[first + k, :, r] + rx[0, :, r] + rx[1, :, r] + rx[2, :, r]
            await_all(late[part], f"late{leap}")
            sum_late = pf[second + k, :, r] + rx[3, :, r] + rx[4, :, r] + rx[5, :, r]
            line[:, r] = jnp.where(core == 0, sum_late, sum_early)
            home.append(go(leap, part, 26, line.at[:, r], rl.at[:, r], at_y(2)))
            keep.append(jnp.where(core == 0, sum_early, sum_late) + tf[2, :, r])
        line_in, own_in, tower_in = [], [], []
        for part in parts:
            r = rows(part)
            await_all(rows_in[part], f"rrows{leap}")
            force = keep[part] + rt[0, :, r] + rt[1, :, r] + rt[2, :, r] + rt[3, :, r]
            await_all([home[part]], f"home{leap}")
            force = force + rl[:, r]
            speed = now[1, :, r] + time_step * force
            place = now[0, :, r] + time_step * speed
            if leap == 0:
                now[1, :, r] = speed
                now[0, :, r] = place
                plate1[k, :, r] = place
                tower1[2, :, r] = place
                line_in.append(send_line(1, part, plate1))
                own_in.append(send_over(1, part, plate1, 5, k))
                tower_in.append(send_tower(1, part, plate1, tower1))
            else:
                out_vel[:, r] = speed
                out_pos[:, r] = place
    with jax.named_scope("sends"):
        for copy in started:
            copy.wait_send()


def shards(positions, velocities, strength, tower_slots, plate_slots, pair_count):
    vm = pl.BlockSpec(memory_space=pltpu.VMEM)
    sm = pl.BlockSpec(memory_space=pltpu.SMEM)
    block = (3, CL, CS)
    scratch = []
    for shape in ((12, 4, CL, CS), (12, *block), (5, 4, CL, CS), (5, *block)):
        scratch.append(pltpu.VMEM(shape, F32))
    for blocks in (12, 5, 4, 4, 6):
        scratch += [pltpu.VMEM((blocks, *block), F32)] * 2
    scratch += [pltpu.VMEM(block, F32)] * 4
    scratch += [pltpu.VMEM((3, PAIRS, CS), F32)] * 2
    scratch += [pltpu.VMEM((2, *block), F32)]
    scratch += [pltpu.SemaphoreType.DMA((2, PARTS, COPIES))] * 2
    tower_slots = tower_slots.reshape(1, PAIRS)
    plate_slots = plate_slots.reshape(1, PAIRS)
    new_pos, new_vel = pl.pallas_call(
        kernel,
        out_shape=[jax.ShapeDtypeStruct(block, F32)] * 2,
        in_specs=[vm, vm, vm, sm, sm, sm, vm, vm],
        out_specs=[vm, vm],
        scratch_shapes=scratch,
        compiler_params=pltpu.CompilerParams(collective_id=0, has_side_effects=True),
        name="leapfrog",
    )(
        positions.reshape(block), velocities.reshape(block), strength.reshape(CL, CS),
        tower_slots, plate_slots, pair_count.reshape(1, 1), tower_slots, plate_slots,
    )
    return new_pos[None, None, None], new_vel[None, None, None]


def solution(mesh):
    wide = P("gx", "gy", "gz", None, None, None)
    in_specs = (
        wide, wide, P("gx", "gy", "gz", None, None),
        P("gx", "gy", "gz", None), P("gx", "gy", "gz", None), P("gx", "gy", "gz"),
    )
    return jax.shard_map(
        shards, mesh=mesh, in_specs=in_specs, out_specs=(wide, wide), check_vma=False
    )
```

```python
import jax
import jax.numpy as jnp
from jax import lax
from jax.experimental import pallas as pl
from jax.experimental.pallas import tpu as pltpu
from jax.sharding import PartitionSpec as P

time_step = 0.02
CL = 32
CS = 128
PAIRS = 128
GROUP = 32
PARTS = 2
ROWS = CL // PARTS
MESH = pl.DeviceIdType.MESH
COPIES = 32
F32 = jnp.float32
BF16 = jnp.bfloat16


def rounded(v):
    return v.astype(BF16).astype(F32)


def split3(v):
    a = rounded(v)
    r = v - a
    b = rounded(r)
    return a, b, rounded(r - b)


def features(rows, weight, sub):
    sq = rows * rows
    norm = (sq[0:1] + sq[1:2] + sq[2:3]) * 0.25
    scaled = rows * weight
    high = rounded(scaled)
    sums = jnp.concatenate([high, scaled - high], axis=0).astype(BF16)
    return norm, sums


def gather_side(pos, wts, block, index, shift, sub):
    x = jnp.broadcast_to(pos[block, 0, pl.ds(index, 1), :], (8, CS))
    y = jnp.broadcast_to(pos[block, 1, pl.ds(index, 1), :], (8, CS))
    z = jnp.broadcast_to(pos[block, 2, pl.ds(index, 1), :], (8, CS))
    s = jnp.broadcast_to(wts[block, 3, pl.ds(index, 1), :], (8, CS))
    one = jnp.where(sub == 3, 1.0, 0.0)
    rows = jnp.where(sub == 0, x, jnp.where(sub == 1, y, jnp.where(sub == 2, z, one)))
    if shift is not None:
        rows = rows + shift
    return rows, s


def one_pair(n, tower, wt_tower, plate, wt_plate, t_slots, p_slots, height, sub):
    ts = t_slots[0, n]
    ps = p_slots[0, n]
    t_block = lax.shift_right_logical(ts, 5)
    t_index = lax.bitwise_and(ts, 31)
    p_block = lax.shift_right_logical(ps, 5)
    p_index = lax.bitwise_and(ps, 31)
    dx = (t_block - 2).astype(F32)
    dy = -lax.shift_right_logical(ps, 7).astype(F32)
    dz = (height - lax.bitwise_and(p_block, 3)).astype(F32)
    shift = jnp.where(sub == 0, dx, jnp.where(sub == 1, dy, jnp.where(sub == 2, dz, 0.0)))
    a, sa = gather_side(tower, wt_tower, t_block, t_index, shift, sub)
    q, sq = gather_side(plate, wt_plate, p_block, p_index, None, sub)
    norm_a, sums_a = features(a, sa, sub)
    norm_q, sums_q = features(q, sq, sub)
    left = jnp.where(
        sub < 3, 0.5 * a, jnp.where(sub == 3, 1.0 - norm_a, jnp.where(sub == 4, 1.0, 0.0))
    )
    right = jnp.where(sub == 4, -norm_q, q)
    a1, a2, a3 = split3(left)
    q1, q2, q3 = split3(right)
    lhs = jnp.concatenate([a1, a1, a2, a1, a3, a2], axis=0)
    rhs = jnp.concatenate([q1, q2, q1, q3, q1, q2], axis=0)
    return dict(a=a, sa=sa, q=q, sq=sq, sums_a=sums_a, sums_q=sums_q, lhs=lhs, rhs=rhs)


def dot(a, b, dims):
    return lax.dot_general(a, b, (dims, ((), ())), preferred_element_type=F32)


def beside(u, v):
    lhs = jnp.concatenate([u["lhs"], v["lhs"]], axis=0).T.astype(BF16)
    zero = jnp.zeros((48, CS), F32)
    rhs = jnp.concatenate(
        [jnp.concatenate([u["rhs"], zero], axis=1), jnp.concatenate([zero, v["rhs"]], axis=1)],
        axis=0,
    ).astype(BF16)
    return lhs, rhs


def group_of_pairs(sides, n, fa_ref, fq_ref):
    twos = [sides[w : w + 2] for w in range(0, len(sides), 2)]
    products = [beside(u, v) for u, v in twos]
    ts = [dot(lhs, rhs, ((1,), (0,))) for lhs, rhs in products]
    outs = []
    for (u, v), t in zip(twos, ts):
        m = jnp.maximum(t, 0.0)
        m = (m * m).astype(BF16)
        wa = jnp.concatenate([u["sums_a"], v["sums_a"]], axis=0)
        wq = jnp.concatenate([u["sums_q"], v["sums_q"]], axis=0)
        stacked = jnp.concatenate([m[:, :CS], m[:, CS:]], axis=0)
        outs.append((dot(wq, stacked, ((1,), (1,))), dot(wa, m, ((1,), (0,)))))
    for w, side in enumerate(sides):
        half = w % 2
        cols = slice(half * CS, (half + 1) * CS)
        on_a, on_q = outs[w // 2]
        for rows, weight, out, ref in (
            (side["a"], side["sa"], on_a, fa_ref),
            (side["q"], side["sq"], on_q, fq_ref),
        ):
            got = out[16 * half : 16 * half + 8, cols] + out[16 * half + 8 : 16 * half + 16, cols]
            force = (rows * got[3:4] - got) * (4.0 * weight)
            for c in range(3):
                ref[c, pl.ds(n + w, 1), :] = force[c : c + 1]


def spread(pair_forces, slots, live, count, out_ref, blocks):
    rows = blocks * CL
    which = lax.broadcasted_iota(jnp.int32, (rows, PAIRS), 0)
    pick = jnp.where((which == slots) & (live < count), 1.0, 0.0).astype(BF16)
    pick = jnp.concatenate([pick, pick], axis=1)
    for c in range(3):
        v = pair_forces[c]
        high = rounded(v)
        both = jnp.concatenate([high, v - high], axis=0).astype(BF16)
        out_ref[:, c] = dot(pick, both, ((1,), (0,))).reshape(blocks, CL, CS)


def kernel(
    pos_ref, vel_ref, str_ref, ts_ref, ps_ref, cnt_ref, tv_ref, pv_ref,
    out_pos, out_vel,
    plate0, plate1, tower0, tower1, pf0, pf1, tf0, tf1, rt0, rt1, rd0, rd1, rx0, rx1,
    line0, line1, rl0, rl1, fa_ref, fq_ref, now, total, send, recv,
):
    i = lax.axis_index("gx")
    j = lax.axis_index("gy")
    k = lax.axis_index("gz")
    nx, ny, nz = lax.axis_size("gx"), lax.axis_size("gy"), lax.axis_size("gz")
    last = nx - 1
    core = lax.rem(j, 2)
    back = lax.rem(j - 2 + ny, ny)
    on = lax.rem(j + 2, ny)
    at_x = lambda d: {"gx": lax.rem(i + d + nx, nx)}
    at_z = lambda d: {"gz": lax.rem(k + d + nz, nz)}
    partner = {"gy": j + 1 - 2 * core}
    is_first, is_second = i == 0, i == 1
    inner = (i >= 1) & (i <= last - 1)
    is_late = i >= last - 1

    barrier = pltpu.get_barrier_semaphore()
    peers = [at_x(d) for d in (-2, -1, 1, 2)] + [{"gy": back}, {"gy": on}, partner]
    peers += [at_z(d) for d in (1, 2, 3)]

    def greet(peer):
        pl.semaphore_signal(barrier, inc=1, device_id=peer, device_id_type=MESH)

    for peer in peers:
        greet(peer)

    plate0[k, 0:3] = pos_ref[...]
    plate0[k, 3] = str_ref[...]
    tower0[2, 0:3] = pos_ref[...]
    tower0[2, 3] = str_ref[...]
    now[0] = pos_ref[...]
    now[1] = vel_ref[...]
    with jax.named_scope("barrier"):
        pl.semaphore_wait(barrier, len(peers))

    sub = lax.broadcasted_iota(jnp.int32, (8, CS), 0)
    live = lax.broadcasted_iota(jnp.int32, (1, PAIRS), 1)
    count = cnt_ref[0, 0]
    started = []

    def when(cond, what):
        if cond is None:
            what()
        else:
            pl.when(cond)(what)

    def copy_of(at, number, src, dst, where, to=None):
        return pltpu.make_async_remote_copy(
            src_ref=src, dst_ref=dst,
            send_sem=send.at[*at, number], recv_sem=recv.at[*at, number if to is None else to],
            device_id=where, device_id_type=MESH,
        )

    def go(*args, cond=None, to=None):
        copy = copy_of(*args, to=to)
        when(cond, copy.start)
        started.append((cond, copy))
        return copy

    def arrived(at, number, ref):
        copy_of(at, number, ref, ref, partner).wait_recv()

    def rows(part):
        return pl.ds(part * ROWS, ROWS)

    def await_all(copies, name):
        for copy in copies:
            with jax.named_scope(name):
                copy.wait_recv()

    def send_own(at, plate, tower):
        r = rows(at[1])
        own, far = plate.at[k, :, r], plate.at[2 * nz + k, :, r]
        line = go(at, 0, own, far, {"gy": back})
        go(at, 6, own, tower.at[0, :, r], {"gx": lax.rem(i + 2, nx)}, cond=is_late, to=1)
        over = [go(at, 8 + d, own, plate.at[k, :, r], at_z(d + 1)) for d in range(3)]
        go(at, 1, own, tower.at[3, :, r], at_x(-1), cond=i >= 1, to=3)
        go(at, 2, own, tower.at[1, :, r], at_x(1), cond=i <= last - 1, to=2)
        go(at, 3, own, tower.at[4, :, r], at_x(-2), cond=i <= 1, to=4)
        return line, over

    def pass_on(at, tower, cond, number, slot, sends, to_slot, step, to):
        row = lambda b: tower.at[b, :, rows(at[1])]
        copy = copy_of(at, sends, row(slot), row(to_slot), at_x(step), to=to)

        @pl.when(cond)
        def _():
            arrived(at, number, row(slot))
            copy.start()

        started.append((cond, copy))

    def rest_of_tower(leap, tower):
        with jax.named_scope(f"tower{leap}"):
            for part in parts:
                at = (leap, part)
                for cond, number, slot in (
                    (is_first | (i >= 2), 1, 0), (is_first | (i == last), 2, 1),
                    (is_first | (i == last), 3, 3), ((i < last - 1) | (i == last), 4, 4),
                ):

                    @pl.when(cond)
                    def _(at=at, number=number, slot=slot, part=part):
                        arrived(at, number, tower.at[slot, :, rows(part)])

    def send_far(at, plate):
        far = plate.at[2 * nz + k, :, rows(at[1])]
        return [go(at, 11 + d, far, far, at_z(d + 1)) for d in range(3)]

    def shared(at, plate, d):
        height = lax.rem(k - d + nz, nz)
        r = rows(at[1])
        return copy_of(
            at, 14 + d,
            plate.at[2 * nz * (1 - core) + height, :, r], plate.at[nz + height, :, r], partner,
        )

    def share_if(who, *args):
        when(core == who, lambda: shared(*args).start())

    parts = range(PARTS)
    own_in = [send_own((0, part), plate0, tower0) for part in parts]
    for leap in range(2):
        plate, tower = ((plate0, tower0), (plate1, tower1))[leap]
        pf, tf = ((pf0, tf0), (pf1, tf1))[leap]
        rt, rd, rx = ((rt0, rd0, rx0), (rt1, rd1, rx1))[leap]
        line, rl = ((line0, rl0), (line1, rl1))[leap]

        for part in parts:
            share_if(1, (leap, part), plate, 0)
        for part in parts:
            for d in range(3):
                await_all([own_in[part][1][d]], f"own{leap}")
                share_if(1, (leap, part), plate, d + 1)
        with jax.named_scope(f"relay{leap}"):
            for part in parts:
                pass_on((leap, part), tower, inner, 2, 1, 4, 0, 1, 1)
                pass_on((leap, part), tower, inner, 3, 3, 5, 4, -1, 4)
        far_in = []
        for part in parts:
            await_all([own_in[part][0]], f"line{leap}")
            far_in.append(send_far((leap, part), plate))
            share_if(0, (leap, part), plate, 0)
        with jax.named_scope(f"wrap{leap}"):
            for part in parts:
                pass_on((leap, part), tower, is_second, 1, 0, 7, 1, -1, 2)
                pass_on((leap, part), tower, i == last - 1, 4, 4, 7, 3, 1, 3)
        for part in parts:
            for d in range(3):
                await_all([far_in[part][d]], f"far{leap}")
                share_if(0, (leap, part), plate, d + 1)
        between = [shared((leap, part), plate, d) for part in parts for d in range(nz)]
        started += [(None, copy) for copy in between]
        await_all(between, f"mid{leap}")
        rest_of_tower(leap, tower)

        def pairs(g, carry, tower=tower, plate=plate):
            base = g * GROUP
            sides = [
                one_pair(base + w, tower, tower0, plate, plate0, ts_ref, ps_ref, k, sub)
                for w in range(GROUP)
            ]
            group_of_pairs(sides, base, fa_ref, fq_ref)
            return carry

        with jax.named_scope(f"pairs{leap}"):
            lax.fori_loop(0, PAIRS // GROUP, pairs, 0)
        with jax.named_scope(f"spread{leap}"):
            spread(fq_ref, pv_ref[...], live, count, pf, 3 * 4)
            spread(fa_ref, tv_ref[...], live, count, tf, 5)

        odd, even = core == 1, core == 0
        second = 2 * nz * (1 - core)

        def over(at, number, block, slot, cond=None, pf=pf, rx=rx):
            r = rows(at[1])
            return [
                go(
                    at, number + d, pf.at[block + lax.rem(k + d + 1, nz), :, r],
                    rx.at[slot + d, :, r], at_z(d + 1), cond=cond,
                )
                for d in range(3)
            ]

        mid, far_home, near_home, home, keep = [], [], [], [], []
        for part in parts:
            at, r = (leap, part), rows(part)
            mid.append(go(at, 18, pf.at[pl.ds(nz, nz), :, r], rd.at[:, :, r], partner))
            over(at, 19, 2 * nz, 0, cond=odd)
            row = lambda n, ref, r=r: ref.at[n, :, r]
            go(at, 25, row(4, tf), row(0, rt), at_x(1), cond=i < last - 1)
            go(at, 26, row(0, tf), row(1, rt), at_x(-1), cond=i >= 2)
            go(at, 29, row(1, tf), row(4, rt), at_x(1), cond=is_first)
            go(at, 29, row(3, tf), row(4, rt), at_x(-1), cond=i == last)
            go(at, 30, row(0, tf), row(5, rt), at_x(-2), cond=is_first)
            go(at, 30, row(4, tf), row(5, rt), at_x(2), cond=i == last)
            go(at, 27, row(3, tf), row(2, rt), at_x(1), cond=is_first)
            go(at, 28, row(1, tf), row(3, rt), at_x(-1), cond=i == last)
        for part in parts:
            at, r = (leap, part), rows(part)
            await_all([mid[part]], f"rmid{leap}")
            pf[pl.ds(second, nz), :, r] = pf[pl.ds(second, nz), :, r] + rd[:, :, r]
            far_home.append(over(at, 19, 2 * nz, 0, cond=even))
        for part in parts:
            near_home.append(over((leap, part), 22, 0, 3))
        for part in parts:
            at, r = (leap, part), rows(part)
            await_all(far_home[part], f"rfar{leap}")
            line[:, r] = pf[2 * nz + k, :, r] + rx[0, :, r] + rx[1, :, r] + rx[2, :, r]
            home.append(go(at, 31, line.at[:, r], rl.at[:, r], {"gy": on}))

        def add_and_pass(at, cond, number, got, slot, sends, to_slot, step, tf=tf, rt=rt):
            r = rows(at[1])
            copy = copy_of(at, sends, tf.at[slot, :, r], rt.at[to_slot, :, r], at_x(step))

            @pl.when(cond)
            def _():
                arrived(at, number, rt.at[got, :, r])
                tf[slot, :, r] = tf[slot, :, r] + rt[got, :, r]
                copy.start()

            started.append((cond, copy))

        with jax.named_scope(f"rsum{leap}"):
            for part in parts:
                at = (leap, part)
                add_and_pass(at, is_second, 29, 4, 0, 30, 5, -2)
                add_and_pass(at, i == last - 1, 29, 4, 4, 30, 5, 2)
                add_and_pass(at, inner, 25, 0, 3, 27, 2, 1)
                add_and_pass(at, inner, 26, 1, 1, 28, 3, -1)
        for part in parts:
            at, r = (leap, part), rows(part)
            await_all(near_home[part], f"rnear{leap}")
            keep.append(pf[k, :, r] + rx[3, :, r] + rx[4, :, r] + rx[5, :, r] + tf[2, :, r])
        own_in = []
        for part in parts:
            at, r = (leap, part), rows(part)
            total[...] = keep[part]
            with jax.named_scope(f"rrows{leap}"):
                for cond, number, slot in (
                    (i >= 1, 27, 2), (i <= last - 1, 28, 3), ((i <= 1) | is_late, 30, 5)
                ):

                    @pl.when(cond)
                    def _(at=at, number=number, slot=slot, r=r, rt=rt):
                        arrived(at, number, rt.at[slot, :, r])
                        total[...] = total[...] + rt[slot, :, r]

            await_all([home[part]], f"home{leap}")
            force = total[...] + rl[:, r]
            speed = now[1, :, r] + time_step * force
            place = now[0, :, r] + time_step * speed
            if leap == 0:
                now[1, :, r] = speed
                now[0, :, r] = place
                plate1[k, :, r] = place
                tower1[2, :, r] = place
                own_in.append(send_own((1, part), plate1, tower1))
            else:
                out_vel[:, r] = speed
                out_pos[:, r] = place
    with jax.named_scope("sends"):
        for cond, copy in started:
            when(cond, copy.wait_send)


def shards(positions, velocities, strength, tower_slots, plate_slots, pair_count):
    vm = pl.BlockSpec(memory_space=pltpu.VMEM)
    sm = pl.BlockSpec(memory_space=pltpu.SMEM)
    block = (3, CL, CS)
    scratch = []
    for shape in ((12, 4, CL, CS), (12, *block), (5, 4, CL, CS), (5, *block)):
        scratch.append(pltpu.VMEM(shape, F32))
    for blocks in (12, 5, 6, 4, 6):
        scratch += [pltpu.VMEM((blocks, *block), F32)] * 2
    scratch += [pltpu.VMEM(block, F32)] * 4
    scratch += [pltpu.VMEM((3, PAIRS, CS), F32)] * 2
    scratch += [pltpu.VMEM((2, *block), F32), pltpu.VMEM((3, ROWS, CS), F32)]
    scratch += [pltpu.SemaphoreType.DMA((2, PARTS, COPIES))] * 2
    tower_slots = tower_slots.reshape(1, PAIRS)
    plate_slots = plate_slots.reshape(1, PAIRS)
    new_pos, new_vel = pl.pallas_call(
        kernel,
        out_shape=[jax.ShapeDtypeStruct(block, F32)] * 2,
        in_specs=[vm, vm, vm, sm, sm, sm, vm, vm],
        out_specs=[vm, vm],
        scratch_shapes=scratch,
        compiler_params=pltpu.CompilerParams(collective_id=0, has_side_effects=True),
        name="leapfrog",
    )(
        positions.reshape(block), velocities.reshape(block), strength.reshape(CL, CS),
        tower_slots, plate_slots, pair_count.reshape(1, 1), tower_slots, plate_slots,
    )
    return new_pos[None, None, None], new_vel[None, None, None]


def solution(mesh):
    wide = P("gx", "gy", "gz", None, None, None)
    in_specs = (
        wide, wide, P("gx", "gy", "gz", None, None),
        P("gx", "gy", "gz", None), P("gx", "gy", "gz", None), P("gx", "gy", "gz"),
    )
    return jax.shard_map(
        shards, mesh=mesh, in_specs=in_specs, out_specs=(wide, wide), check_vma=False
    )
```
